32 devices in a mesh: row: 8 (over z, x), col: 4 (over y, core).
Axes of the slice: x: 2, y: 2, z: 4, core: 2. Of those that a mesh axis runs over, the one named last changes fastest.
Arguments:
- diag_tiles: float32 [8, 512, 512], P('row', 'col'), as said below
- sub_tiles: float32 [8, 512, 512], P('row', 'col')
- boundary: float32 [512, 512], P('col'), as said below
Outputs:
- inverse_blocks: float32 [8, 512, 512], P('row', 'col')
Inputs may be any that keep to these rules, and one draw needn't show every extreme that they name: `diag_tiles`: every tile is lower triangular, zero above the diagonal, with diagonal entries between 0.2 and 0.4. `boundary`: symmetric positive definite, smallest eigenvalue at least 2.
All inputs are finite; a program needn't handle non-finite values.
Results may differ from the reference program's by a relative error of at most 0.0003.
Values sent between devices are 32-bit elements; how exact they have to be, the bound alone decides.
A program may use at most 256 MiB of HBM per device.

```python
import math
import jax
import jax.numpy as jnp
from jax import lax

B = 512
NBLK = 8


def draw_diag_tiles(key, part):
    first_key = jax.random.fold_in(key, 11)
    second_key = jax.random.fold_in(key, 12)
    diagonal = jnp.exp(jax.random.uniform(first_key, (NBLK, B), jnp.float32, math.log(0.2), math.log(0.4)))
    below = jax.random.normal(second_key, (NBLK, B, B), jnp.float32) * (0.1 / math.sqrt(B))
    strict_mask = jnp.tril(jnp.ones((B, B), jnp.float32), -1)
    identity = jnp.eye(B, dtype=jnp.float32)
    return below * strict_mask + diagonal[:, :, None] * identity


def invert_lower(tile):
    return jax.scipy.linalg.solve_triangular(tile, jnp.eye(B, dtype=jnp.float32), lower=True)


def draw_sub_tiles(key, part):
    inverse_tiles = draw_diag_tiles(key, part)
    lower = jax.vmap(invert_lower)(inverse_tiles)
    orth_key = jax.random.fold_in(key, 21)
    rate_key = jax.random.fold_in(key, 22)
    gauss = jax.random.normal(orth_key, (NBLK, B, B), jnp.float32)
    orthogonal, triangle = jnp.linalg.qr(gauss)
    rates = jax.random.uniform(rate_key, (NBLK,), jnp.float32, 0.5, 1.5)
    gains = jnp.exp(-rates / NBLK)
    coupled = jnp.einsum('kij,kjl->kil', orthogonal, lower, precision=lax.Precision.HIGHEST)
    return gains[:, None, None] * coupled


def draw_boundary(key, part):
    inner_key = jax.random.fold_in(key, 31)
    scale_key = jax.random.fold_in(key, 32)
    factor = jax.random.normal(inner_key, (B, B), jnp.float32)
    level = jnp.exp(jax.random.uniform(scale_key, (), jnp.float32, math.log(2.0), math.log(6.0)))
    gram = jnp.dot(factor, factor.T, precision=lax.Precision.HIGHEST) / B
    return level * (gram + jnp.eye(B, dtype=jnp.float32))


def setup_inputs(seed: int = 0) -> dict:
    key_list = jax.random.split(jax.random.key(seed), 4)
    return {
        "diag_tiles": draw_diag_tiles(jax.random.fold_in(key_list[3], 71), 0),
        "sub_tiles": draw_sub_tiles(jax.random.fold_in(key_list[3], 71), 0),
        "boundary": draw_boundary(jax.random.fold_in(key_list[3], 71), 0),
    }


def product(left, right):
    return jnp.dot(left, right, precision=lax.Precision.HIGHEST)

def reference(diag_tiles, sub_tiles, boundary):

    def step(z_next, tiles):
        tile_inverse, coupling = tiles
        local_term = product(tile_inverse.T, tile_inverse)
        weight = product(coupling, tile_inverse)
        z_here = local_term + product(weight.T, product(z_next, weight))
        return (z_here, z_here)
    final_block, inverse_blocks = lax.scan(step, boundary, (diag_tiles, sub_tiles), reverse=True)
    return inverse_blocks
```

```python
import functools
import jax
import jax.numpy as jnp
from jax import lax
from jax.experimental import pallas as pl
from jax.experimental.pallas import tpu as pltpu
from jax.sharding import PartitionSpec as P

MESH = pl.DeviceIdType.MESH
F32 = jnp.float32
BF16 = jnp.bfloat16
LANES = 128


def split(x):
    high = x.astype(BF16)
    return high, (x - high.astype(F32)).astype(BF16)


def mm(a, b, transposed=False):
    (ah, al), (bh, bl) = a, b
    dims = (((1,), (1 if transposed else 0,)), ((), ()))
    dot = lambda l, r: lax.dot_general(l, r, dims, preferred_element_type=F32)
    m = ah.shape[0]
    both = dot(jnp.concatenate([ah, al], axis=0), bh)
    return both[:m] + (both[m:] + dot(ah, bl))


def kernel(rows_n, cols_n, t_in, s_in, e_in, out, t_all, s_all, zbuf, th, tl, wf, wh, wl,
           mf, mh, ml, zh, zl, sc, lo, zes, send, recv, local):
    row, c = lax.axis_index("row"), lax.axis_index("col")
    p, level = lax.rem(row, 2), row // 2
    core, y = lax.rem(c, 2), c // 2
    ny = cols_n // 2
    R, B = t_in.shape[1], t_in.shape[2]
    levels = rows_n // 2
    top = level == levels - 1
    other_y = [lax.rem(y + d, ny) for d in range(1, ny)]
    across = (row + 1 - 2 * p, c)
    partner = (row, c + 1 - 2 * core)
    beside = [(row, v * 2 + core) for v in other_y]

    barrier = pltpu.get_barrier_semaphore()
    greet = [across, partner] + beside
    for d in greet:
        pl.semaphore_signal(barrier, inc=1, device_id=d, device_id_type=MESH)

    @pl.when(level > 0)
    def _():
        pl.semaphore_signal(barrier, inc=1, device_id=(row - 2, c), device_id_type=MESH)

    @pl.when(jnp.logical_not(top))
    def _():
        pl.semaphore_signal(barrier, inc=1, device_id=(row + 2, c), device_id_type=MESH)

    above, below = levels - 1 - level, level
    peers = (above + levels - 1) // levels + (below + levels - 1) // levels
    pl.semaphore_wait(barrier, len(greet) + peers)

    bufs = (t_all, s_all, zbuf)

    def chunk(a, pp, cc, h):
        if a < 2:
            return bufs[a].at[pp, pl.ds(pl.multiple_of(cc * R + h * (R // 2), 8), R // 2), :]
        start = cc * R + pp * (R // 2) + h * (R // 4)
        return zbuf.at[pl.ds(pl.multiple_of(start, 8), R // 4), :]

    started = []
    count = [0]

    def copy(src, a, pp, cc, h, dev):
        d = pltpu.make_async_remote_copy(
            src_ref=src, dst_ref=chunk(a, pp, cc, h), send_sem=send.at[count[0]],
            recv_sem=recv.at[a, pp, cc, h], device_id=dev, device_id_type=MESH)
        count[0] += 1
        return d

    def launch(src, a, pp, cc, h, dev):
        d = copy(src, a, pp, cc, h, dev)
        d.start()
        started.append(d)

    def arrived(a, pp, cc, h):
        ref = chunk(a, pp, cc, h)
        pltpu.make_async_remote_copy(
            src_ref=ref, dst_ref=ref, send_sem=send.at[0], recv_sem=recv.at[a, pp, cc, h],
            device_id=partner, device_id_type=MESH).wait_recv()

    def own_copies(src, a):
        return [copy(src(h), a, p, c, h, d) for h in range(2) for d in [across] + beside + [partner]]

    def forward(a):
        q = 1 - p
        for h in range(2):
            arrived(a, q, c, h)
            if h == 0:
                for d in beside:
                    launch(chunk(a, q, c, h), a, q, c, h, d)
            launch(chunk(a, q, c, h), a, q, c, h, partner)
            for d in beside:
                arrived(a, p, d[1], h)
                if h == 1:
                    launch(chunk(a, p, d[1], h), a, p, d[1], h, across)
                launch(chunk(a, p, d[1], h), a, p, d[1], h, partner)

    def finish(a):
        q = 1 - p
        for h in range(2):
            for d in beside:
                arrived(a, q, d[1], h)
                launch(chunk(a, q, d[1], h), a, q, d[1], h, partner)
        for h in range(2):
            for v in [y] + other_y:
                cc = v * 2 + 1 - core
                arrived(a, p, cc, h)
                arrived(a, q, cc, h)

    for a, ref in ((0, t_in), (1, s_in)):
        for d in own_copies(lambda h: ref.at[0, pl.ds(h * (R // 2), R // 2), :], a):
            d.start()
            started.append(d)
    here = pl.ds(pl.multiple_of(c * R, 8), R)
    keep = [pltpu.make_async_copy(t_in.at[0], t_all.at[p, here, :], local.at[0]),
            pltpu.make_async_copy(s_in.at[0], s_all.at[p, here, :], local.at[1])]
    for d in keep:
        d.start()

    z_own = own_copies(lambda h: chunk(2, p, c, h), 2)
    started.extend(z_own)

    @pl.when(top)
    def _():
        mine = pltpu.make_async_copy(
            e_in.at[pl.ds(pl.multiple_of(p * (R // 2), 8), R // 2), :],
            zbuf.at[pl.ds(pl.multiple_of(c * R + p * (R // 2), 8), R // 2), :], local.at[2])
        mine.start()
        mine.wait()
        for d in z_own:
            d.start()

    for d in keep:
        d.wait()
    forward(0)
    finish(0)
    forward(1)
    for k in range(2):
        th[k], tl[k] = split(t_all[k])
    finish(1)

    def weight(i, _):
        k, at = i // (B // LANES), pl.ds(pl.multiple_of(lax.rem(i, B // LANES) * LANES, LANES), LANES)
        w = mm(split(s_all[k, at, :]), (th[k], tl[k]))
        wf[k, at, :] = w
        wh[k, at, :], wl[k, at, :] = split(w)
        return 0

    lax.fori_loop(0, 2 * (B // LANES), weight, 0)

    def joined(i, _):
        at = pl.ds(pl.multiple_of(i * LANES, LANES), LANES)
        m = mm((wh[1, at, :], wl[1, at, :]), (wh[0], wl[0]))
        mf[at, :] = m
        mh[at, :], ml[at, :] = split(m)
        return 0

    lax.fori_loop(0, B // LANES, joined, 0)

    base = pl.ds(pl.multiple_of((c * R) // LANES * LANES, LANES), LANES)
    off = lax.rem(c * R, LANES)
    turned = mm(split(wf[0, :, base].T), (th[1], tl[1]), transposed=True)
    turned = mm(split(turned), (th[1], tl[1]))
    sc[...] = mm(split(turned), (wh[0], wl[0])) + mm(split(t_all[0, :, base].T), (th[0], tl[0]))
    lo[...] = mm(split(t_all[1, :, base].T), (th[1], tl[1]))

    @pl.when(jnp.logical_not(top))
    def _():
        for h in range(2):
            arrived(2, p, c, h)
            for d in z_own[h * (len(z_own) // 2):(h + 1) * (len(z_own) // 2)]:
                d.start()

    forward(2)
    finish(2)
    zh[...], zl[...] = split(zbuf[...])
    mt = split(mf[:, base].T)
    moved = mm(mt, (zh[...], zl[...]))
    zes[...] = sc[...] + mm(split(moved), (mh[...], ml[...]))

    down = []
    for h in range(2):
        src = zes.at[pl.ds(pl.multiple_of(off + p * (R // 2) + h * (R // 4), 8), R // 4), :]
        down.append(copy(src, 2, p, c, h, (row - 2, c)))

    @pl.when(level > 0)
    def _():
        for d in down:
            d.start()

    rows = pl.ds(pl.multiple_of(off, 8), R)

    @pl.when(p == 0)
    def _():
        out[0] = zes[rows, :]

    @pl.when(p == 1)
    def _():
        step = mm(split(wf[1, :, base].T), (zh[...], zl[...]))
        lo[...] = lo[...] + mm(split(step), (wh[1], wl[1]))
        out[0] = lo[rows, :]

    for d in started:
        d.wait_send()

    @pl.when(level > 0)
    def _():
        for d in down:
            d.wait_send()


def solution(mesh):
    rows_n, cols_n = mesh.shape["row"], mesh.shape["col"]

    def on_device(t, s, e):
        R, B = t.shape[1], t.shape[2]
        ny = cols_n // 2
        sends = 3 * (2 * (ny + 1) + (ny - 1) + 2 + 5 * (ny - 1)) + 2
        vmem = pl.BlockSpec(memory_space=pltpu.VMEM)
        V = pltpu.VMEM
        return pl.pallas_call(
            functools.partial(kernel, rows_n, cols_n),
            out_shape=jax.ShapeDtypeStruct(t.shape, F32),
            in_specs=[vmem] * 3,
            out_specs=vmem,
            scratch_shapes=[
                V((2, B, B), F32), V((2, B, B), F32), V((B, B), F32),
                V((2, B, B), BF16), V((2, B, B), BF16),
                V((2, B, B), F32), V((2, B, B), BF16), V((2, B, B), BF16),
                V((B, B), F32), V((B, B), BF16), V((B, B), BF16),
                V((B, B), BF16), V((B, B), BF16),
                V((LANES, B), F32), V((LANES, B), F32), V((LANES, B), F32),
                pltpu.SemaphoreType.DMA((sends,)),
                pltpu.SemaphoreType.DMA((3, 2, cols_n, 2)),
                pltpu.SemaphoreType.DMA((3,)),
            ],
            compiler_params=pltpu.CompilerParams(collective_id=0, has_side_effects=True,
                                                 vmem_limit_bytes=56 * 2**20),
        )(t, s, e)

    return jax.shard_map(
        on_device, mesh=mesh,
        in_specs=(P("row", "col", None), P("row", "col", None), P("col", None)),
        out_specs=P("row", "col", None), check_vma=False)
```

```python
import functools
import jax
import jax.numpy as jnp
from jax import lax
from jax.experimental import pallas as pl
from jax.experimental.pallas import tpu as pltpu
from jax.sharding import PartitionSpec as P

MESH = pl.DeviceIdType.MESH
F32 = jnp.float32
BF16 = jnp.bfloat16
LANES = 128


def split(x):
    high = x.astype(BF16)
    return high, (x - high.astype(F32)).astype(BF16)


def mm(a, b, transposed=False):
    (ah, al), (bh, bl) = a, b
    dims = (((1,), (1 if transposed else 0,)), ((), ()))
    dot = lambda l, r: lax.dot_general(l, r, dims, preferred_element_type=F32)
    m = ah.shape[0]
    both = dot(jnp.concatenate([ah, al], axis=0), bh)
    return both[:m] + (both[m:] + dot(ah, bl))


def kernel(rows_n, cols_n, t_in, s_in, e_in, out, t_all, s_all, zbuf, th, tl, wf, wh, wl,
           mf, mh, ml, zh, zl, sc, lo, zes, mbuf, sbuf, folded, send, recv, local):
    row, c = lax.axis_index("row"), lax.axis_index("col")
    p, level = lax.rem(row, 2), row // 2
    core, y = lax.rem(c, 2), c // 2
    ny = cols_n // 2
    R, B = t_in.shape[1], t_in.shape[2]
    levels = rows_n // 2
    top = level == levels - 1
    other_y = [lax.rem(y + d, ny) for d in range(1, ny)]
    across = (row + 1 - 2 * p, c)
    partner = (row, c + 1 - 2 * core)
    beside = [(row, v * 2 + core) for v in other_y]

    barrier = pltpu.get_barrier_semaphore()
    greet = [across, partner] + beside
    for d in greet:
        pl.semaphore_signal(barrier, inc=1, device_id=d, device_id_type=MESH)

    @pl.when(level > 0)
    def _():
        pl.semaphore_signal(barrier, inc=1, device_id=(row - 2, c), device_id_type=MESH)

    @pl.when(jnp.logical_not(top))
    def _():
        pl.semaphore_signal(barrier, inc=1, device_id=(row + 2, c), device_id_type=MESH)

    above, below = levels - 1 - level, level
    peers = (above + levels - 1) // levels + (below + levels - 1) // levels
    pl.semaphore_wait(barrier, len(greet) + peers)

    bufs = (t_all, s_all, zbuf, mbuf, sbuf)
    odd_level = lax.rem(level, 2) == 1
    feeds = jnp.logical_and(odd_level, jnp.logical_not(top))
    fed = jnp.logical_and(jnp.logical_not(odd_level), level < levels - 2)
    sends_z = jnp.logical_and(level > 0, jnp.logical_not(feeds))

    def chunk(a, pp, cc, h):
        if a < 2:
            return bufs[a].at[pp, pl.ds(pl.multiple_of(cc * R + h * (R // 2), 8), R // 2), :]
        start = cc * R + pp * (R // 2) + h * (R // 4)
        return bufs[a].at[pl.ds(pl.multiple_of(start, 8), R // 4), :]

    started = []
    count = [0]

    def copy(src, a, pp, cc, h, dev):
        d = pltpu.make_async_remote_copy(
            src_ref=src, dst_ref=chunk(a, pp, cc, h), send_sem=send.at[count[0]],
            recv_sem=recv.at[a, pp, cc, h], device_id=dev, device_id_type=MESH)
        count[0] += 1
        return d

    def launch(src, a, pp, cc, h, dev):
        d = copy(src, a, pp, cc, h, dev)
        d.start()
        started.append(d)

    def arrived(a, pp, cc, h):
        ref = chunk(a, pp, cc, h)
        pltpu.make_async_remote_copy(
            src_ref=ref, dst_ref=ref, send_sem=send.at[0], recv_sem=recv.at[a, pp, cc, h],
            device_id=partner, device_id_type=MESH).wait_recv()

    def own_copies(src, a):
        return [copy(src(h), a, p, c, h, d) for h in range(2) for d in [across] + beside + [partner]]

    def forward(a, between=lambda: None):
        q = 1 - p
        for h in range(2):
            arrived(a, q, c, h)
            if h == 0:
                for d in beside:
                    launch(chunk(a, q, c, h), a, q, c, h, d)
            launch(chunk(a, q, c, h), a, q, c, h, partner)
            for d in beside:
                arrived(a, p, d[1], h)
                if h == 1:
                    launch(chunk(a, p, d[1], h), a, p, d[1], h, across)
                launch(chunk(a, p, d[1], h), a, p, d[1], h, partner)
            if h == 0:
                between()

    def finish(a, use=lambda pp, cc: None):
        q = 1 - p
        use(q, c)
        for d in beside:
            use(p, d[1])
        for h in range(2):
            for d in beside:
                arrived(a, q, d[1], h)
                launch(chunk(a, q, d[1], h), a, q, d[1], h, partner)
        for pp in (p, q):
            for v in [y] + other_y:
                for h in range(2):
                    arrived(a, pp, v * 2 + 1 - core, h)
                use(pp, v * 2 + 1 - core)
        for d in beside:
            use(q, d[1])

    def start(copies):
        for d in copies:
            d.start()
            started.append(d)

    def drain():
        for d in started:
            d.wait_send()
        started.clear()

    t_own = own_copies(lambda h: t_in.at[0, pl.ds(h * (R // 2), R // 2), :], 0)
    s_own = own_copies(lambda h: s_in.at[0, pl.ds(h * (R // 2), R // 2), :], 1)
    half = len(s_own) // 2
    start(t_own)
    here = pl.ds(pl.multiple_of(c * R, 8), R)
    keep = [pltpu.make_async_copy(t_in.at[0], t_all.at[p, here, :], local.at[0]),
            pltpu.make_async_copy(s_in.at[0], s_all.at[p, here, :], local.at[1])]
    for d in keep:
        d.start()
    forward(0, lambda: start(s_own[:half]))
    start(s_own[half:])
    for d in keep:
        d.wait()
    finish(0)
    for k in range(2):
        th[k], tl[k] = split(t_all[k])

    def weight(pp, cc):
        at = pl.ds(pl.multiple_of(cc * R, 8), R)
        w = mm(split(s_all[pp, at, :]), (th[pp], tl[pp]))
        wf[pp, at, :] = w
        wh[pp, at, :], wl[pp, at, :] = split(w)

    weight(p, c)
    forward(1)
    first_own = own_copies(lambda h: chunk(2, p, c, h), 2)

    @pl.when(top)
    def _():
        mine = pltpu.make_async_copy(
            e_in.at[pl.ds(pl.multiple_of(p * (R // 2), 8), R // 2), :],
            zbuf.at[pl.ds(pl.multiple_of(c * R + p * (R // 2), 8), R // 2), :], local.at[2])
        mine.start()
        mine.wait()
        for d in first_own:
            d.start()

    finish(1, weight)
    outer = list(started)
    started.clear()

    @pl.when(top)
    def _():
        forward(2)
        finish(2)
        started.extend(first_own)
        drain()

    def joined(i, _):
        at = pl.ds(pl.multiple_of(i * LANES, LANES), LANES)
        m = mm((wh[1, at, :], wl[1, at, :]), (wh[0], wl[0]))
        mf[at, :] = m
        mh[at, :], ml[at, :] = split(m)
        return 0

    lax.fori_loop(0, B // LANES, joined, 0)

    base = pl.ds(pl.multiple_of((c * R) // LANES * LANES, LANES), LANES)
    off = lax.rem(c * R, LANES)
    turned = mm(split(wf[0, :, base].T), (th[1], tl[1]), transposed=True)
    turned = mm(split(turned), (th[1], tl[1]))
    sc[...] = mm(split(turned), (wh[0], wl[0])) + mm(split(t_all[0, :, base].T), (th[0], tl[0]))

    def quarter(ref, first, h):
        at = first + p * (R // 2) + h * (R // 4)
        return ref.at[pl.ds(pl.multiple_of(at, 8), R // 4), :]

    below_me = (row - 2, c)
    composite = [copy(quarter(ref, first, h), a, p, c, h, below_me)
                 for a, ref, first in ((3, mf, c * R), (4, sc, off)) for h in range(2)]
    relay = [copy(chunk(2, p, c, h), 2, p, c, h, below_me) for h in range(2)]
    down = [copy(quarter(zes, off, h), 2, p, c, h, below_me) for h in range(2)]

    @pl.when(feeds)
    def _():
        for d in composite:
            d.start()

    lo[...] = mm(split(t_all[1, :, base].T), (th[1], tl[1]))

    @pl.when(fed)
    def _():
        for a in (3, 4):
            own = own_copies(lambda h: chunk(a, p, c, h), a)
            n = len(own) // 2
            for h in range(2):
                arrived(a, p, c, h)
                start(own[h * n:(h + 1) * n])
        for a in (3, 4):
            forward(a)
            finish(a)
        drain()
        zh[...], zl[...] = split(sbuf[...])
        left = mm(split(mf[:, base].T), (zh[...], zl[...]))
        sc[...] = sc[...] + mm(split(left), (mh[...], ml[...]))
        left = mm(split(wf[1, :, base].T), (zh[...], zl[...]))
        lo[...] = lo[...] + mm(split(left), (wh[1], wl[1]))

        def fold(i, _):
            at = pl.ds(pl.multiple_of(i * LANES, LANES), LANES)
            m = split(mbuf[at, :])
            folded[0, at, :] = mm(m, (mh[...], ml[...]))
            folded[1, at, :] = mm(m, (wh[1], wl[1]))
            return 0

        lax.fori_loop(0, B // LANES, fold, 0)

        def place(i, _):
            at = pl.ds(pl.multiple_of(i * LANES, LANES), LANES)
            mf[at, :] = folded[0, at, :]
            mh[at, :], ml[at, :] = split(folded[0, at, :])
            wf[1, at, :] = folded[1, at, :]
            wh[1, at, :], wl[1, at, :] = split(folded[1, at, :])
            return 0

        lax.fori_loop(0, B // LANES, place, 0)

    @pl.when(jnp.logical_not(top))
    def _():
        own = own_copies(lambda h: chunk(2, p, c, h), 2)
        n = len(own) // 2
        for h in range(2):
            arrived(2, p, c, h)

            @pl.when(feeds)
            def _():
                relay[h].start()

            start(own[h * n:(h + 1) * n])
        forward(2)
        finish(2)
        drain()

    zh[...], zl[...] = split(zbuf[...])

    moved = mm(split(mf[:, base].T), (zh[...], zl[...]))
    zes[...] = sc[...] + mm(split(moved), (mh[...], ml[...]))

    @pl.when(sends_z)
    def _():
        for d in down:
            d.start()

    rows = pl.ds(pl.multiple_of(off, 8), R)

    @pl.when(p == 0)
    def _():
        out[0] = zes[rows, :]

    @pl.when(p == 1)
    def _():
        step = mm(split(wf[1, :, base].T), (zh[...], zl[...]))
        lo[...] = lo[...] + mm(split(step), (wh[1], wl[1]))
        out[0] = lo[rows, :]

    for d in outer:
        d.wait_send()

    @pl.when(sends_z)
    def _():
        for d in down:
            d.wait_send()

    @pl.when(feeds)
    def _():
        for d in composite + relay:
            d.wait_send()


def solution(mesh):
    rows_n, cols_n = mesh.shape["row"], mesh.shape["col"]

    def on_device(t, s, e):
        R, B = t.shape[1], t.shape[2]
        ny = cols_n // 2
        sends = 6 * (2 * (ny + 1) + (ny - 1) + 2 + 5 * (ny - 1)) + 8
        vmem = pl.BlockSpec(memory_space=pltpu.VMEM)
        V = pltpu.VMEM
        return pl.pallas_call(
            functools.partial(kernel, rows_n, cols_n),
            out_shape=jax.ShapeDtypeStruct(t.shape, F32),
            in_specs=[vmem] * 3,
            out_specs=vmem,
            scratch_shapes=[
                V((2, B, B), F32), V((2, B, B), F32), V((B, B), F32),
                V((2, B, B), BF16), V((2, B, B), BF16),
                V((2, B, B), F32), V((2, B, B), BF16), V((2, B, B), BF16),
                V((B, B), F32), V((B, B), BF16), V((B, B), BF16),
                V((B, B), BF16), V((B, B), BF16),
                V((LANES, B), F32), V((LANES, B), F32), V((LANES, B), F32),
                V((B, B), F32), V((B, B), F32), V((2, B, B), F32),
                pltpu.SemaphoreType.DMA((sends,)),
                pltpu.SemaphoreType.DMA((5, 2, cols_n, 2)),
                pltpu.SemaphoreType.DMA((3,)),
            ],
            compiler_params=pltpu.CompilerParams(collective_id=0, has_side_effects=True,
                                                 vmem_limit_bytes=56 * 2**20),
        )(t, s, e)

    return jax.shard_map(
        on_device, mesh=mesh,
        in_specs=(P("row", "col", None), P("row", "col", None), P("col", None)),
        out_specs=P("row", "col", None), check_vma=False)
```

```python
import functools
import jax
import jax.numpy as jnp
from jax import lax
from jax.experimental import pallas as pl
from jax.experimental.pallas import tpu as pltpu
from jax.sharding import PartitionSpec as P

MESH = pl.DeviceIdType.MESH
F32 = jnp.float32
BF16 = jnp.bfloat16
LANES = 128


def split(x):
    high = x.astype(BF16)
    return high, (x - high.astype(F32)).astype(BF16)


def mm(a, b, transposed=False):
    (ah, al), (bh, bl) = a, b
    dims = (((1,), (1 if transposed else 0,)), ((), ()))
    dot = lambda l, r: lax.dot_general(l, r, dims, preferred_element_type=F32)
    m = ah.shape[0]
    both = dot(jnp.concatenate([ah, al], axis=0), bh)
    return both[:m] + (both[m:] + dot(ah, bl))


def kernel(rows_n, cols_n, t_in, s_in, e_in, out, t_all, s_all, zbuf, th, tl, wf, wh, wl,
           mf, mh, ml, zh, zl, sc, lo, zes, mbuf, sbuf, folded, send, recv, local):
    row, c = lax.axis_index("row"), lax.axis_index("col")
    p, level = lax.rem(row, 2), row // 2
    core, y = lax.rem(c, 2), c // 2
    ny = cols_n // 2
    R, B = t_in.shape[1], t_in.shape[2]
    levels = rows_n // 2
    top = level == levels - 1
    other_y = [lax.rem(y + d, ny) for d in range(1, ny)]
    across = (row + 1 - 2 * p, c)
    partner = (row, c + 1 - 2 * core)
    beside = [(row, v * 2 + core) for v in other_y]

    barrier = pltpu.get_barrier_semaphore()
    greet = [across, partner] + beside
    for d in greet:
        pl.semaphore_signal(barrier, inc=1, device_id=d, device_id_type=MESH)

    side = row + 1 - 2 * p
    for step, near in ((-2, level > 0), (2, jnp.logical_not(top))):
        @pl.when(near)
        def _():
            pl.semaphore_signal(barrier, inc=1, device_id=(row + step, c), device_id_type=MESH)
            for d in beside:
                pl.semaphore_signal(barrier, inc=1, device_id=(side + step, d[1]), device_id_type=MESH)

    above, below = levels - 1 - level, level
    peers = (above + levels - 1) // levels + (below + levels - 1) // levels
    pl.semaphore_wait(barrier, len(greet) + peers * (1 + len(beside)))

    bufs = (t_all, s_all, zbuf, mbuf, sbuf)
    odd_level = lax.rem(level, 2) == 1
    feeds = jnp.logical_and(odd_level, jnp.logical_not(top))
    fed = jnp.logical_and(jnp.logical_not(odd_level), level < levels - 2)
    sends_z = jnp.logical_and(level > 0, jnp.logical_not(feeds))

    def pieces(a):
        return 2 if a < 2 else max(2, min(4, R // 16))

    def chunk(a, pp, cc, h):
        if a < 2:
            return bufs[a].at[pp, pl.ds(pl.multiple_of(cc * R + h * (R // 2), 8), R // 2), :]
        n = R // 2 // pieces(a)
        return bufs[a].at[pl.ds(pl.multiple_of(cc * R + pp * (R // 2) + h * n, 8), n), :]

    started = []
    count = [0]

    def copy(src, a, pp, cc, h, dev):
        d = pltpu.make_async_remote_copy(
            src_ref=src, dst_ref=chunk(a, pp, cc, h), send_sem=send.at[count[0]],
            recv_sem=recv.at[a, pp, cc, h], device_id=dev, device_id_type=MESH)
        count[0] += 1
        return d

    def launch(src, a, pp, cc, h, dev):
        d = copy(src, a, pp, cc, h, dev)
        d.start()
        started.append(d)

    def arrived(a, pp, cc, h):
        ref = chunk(a, pp, cc, h)
        pltpu.make_async_remote_copy(
            src_ref=ref, dst_ref=ref, send_sem=send.at[0], recv_sem=recv.at[a, pp, cc, h],
            device_id=partner, device_id_type=MESH).wait_recv()

    def own_copies(src, a):
        return [copy(src(h), a, p, c, h, d) for h in range(pieces(a))
                for d in [across] + beside + [partner]]

    def forward(a, between=lambda: None, direct=False):
        q = 1 - p
        for h in range(pieces(a)):
            arrived(a, q, c, h)
            if h % 2 == 0 and not direct:
                for d in beside:
                    launch(chunk(a, q, c, h), a, q, c, h, d)
            launch(chunk(a, q, c, h), a, q, c, h, partner)
            for d in beside:
                arrived(a, p, d[1], h)
                if h % 2 == 1 and not direct:
                    launch(chunk(a, p, d[1], h), a, p, d[1], h, across)
                launch(chunk(a, p, d[1], h), a, p, d[1], h, partner)
            if h == 0:
                between()

    def finish(a, use=lambda pp, cc: None):
        q = 1 - p
        use(q, c)
        for d in beside:
            use(p, d[1])
        for h in range(pieces(a)):
            for d in beside:
                arrived(a, q, d[1], h)
                launch(chunk(a, q, d[1], h), a, q, d[1], h, partner)
        for pp in (p, q):
            for v in [y] + other_y:
                for h in range(pieces(a)):
                    arrived(a, pp, v * 2 + 1 - core, h)
                use(pp, v * 2 + 1 - core)
        for d in beside:
            use(q, d[1])

    def start(copies):
        for d in copies:
            d.start()
            started.append(d)

    def drain():
        for d in started:
            d.wait_send()
        started.clear()

    t_own = own_copies(lambda h: t_in.at[0, pl.ds(h * (R // 2), R // 2), :], 0)
    s_own = own_copies(lambda h: s_in.at[0, pl.ds(h * (R // 2), R // 2), :], 1)
    half = len(s_own) // 2
    start(t_own)
    here = pl.ds(pl.multiple_of(c * R, 8), R)
    keep = [pltpu.make_async_copy(t_in.at[0], t_all.at[p, here, :], local.at[0]),
            pltpu.make_async_copy(s_in.at[0], s_all.at[p, here, :], local.at[1])]
    for d in keep:
        d.start()
    forward(0, lambda: start(s_own[:half]))
    start(s_own[half:])
    for d in keep:
        d.wait()
    finish(0)
    for k in range(2):
        th[k], tl[k] = split(t_all[k])

    def weight(pp, cc):
        at = pl.ds(pl.multiple_of(cc * R, 8), R)
        w = mm(split(s_all[pp, at, :]), (th[pp], tl[pp]))
        wf[pp, at, :] = w
        wh[pp, at, :], wl[pp, at, :] = split(w)

    weight(p, c)
    forward(1)
    first_own = own_copies(lambda h: chunk(2, p, c, h), 2)

    @pl.when(top)
    def _():
        mine = pltpu.make_async_copy(
            e_in.at[pl.ds(pl.multiple_of(p * (R // 2), 8), R // 2), :],
            zbuf.at[pl.ds(pl.multiple_of(c * R + p * (R // 2), 8), R // 2), :], local.at[2])
        mine.start()
        mine.wait()
        for d in first_own:
            d.start()

    finish(1, weight)
    outer = list(started)
    started.clear()

    @pl.when(top)
    def _():
        forward(2)
        finish(2)
        started.extend(first_own)
        drain()

    def joined(i, _):
        at = pl.ds(pl.multiple_of(i * LANES, LANES), LANES)
        m = mm((wh[1, at, :], wl[1, at, :]), (wh[0], wl[0]))
        mf[at, :] = m
        mh[at, :], ml[at, :] = split(m)
        return 0

    lax.fori_loop(0, B // LANES, joined, 0)

    base = pl.ds(pl.multiple_of((c * R) // LANES * LANES, LANES), LANES)
    off = lax.rem(c * R, LANES)
    turned = mm(split(wf[0, :, base].T), (th[1], tl[1]), transposed=True)
    turned = mm(split(turned), (th[1], tl[1]))
    sc[...] = mm(split(turned), (wh[0], wl[0])) + mm(split(t_all[0, :, base].T), (th[0], tl[0]))

    def piece(a, ref, first, h):
        n = R // 2 // pieces(a)
        return ref.at[pl.ds(pl.multiple_of(first + p * (R // 2) + h * n, 8), n), :]

    below_me = (row - 2, c)
    below_diagonal = [(row - 1 - 2 * p, d[1]) for d in beside]
    composite = [copy(piece(a, ref, first, h), a, p, c, h, below_me)
                 for a, ref, first in ((3, mf, c * R), (4, sc, off)) for h in range(pieces(a))]
    relay = [[copy(chunk(2, p, c, h), 2, p, c, h, d) for d in [below_me] + below_diagonal]
             for h in range(pieces(2))]
    down = [copy(piece(2, zes, off, h), 2, p, c, h, d)
            for d in [below_me] + below_diagonal for h in range(pieces(2))]

    @pl.when(feeds)
    def _():
        for d in composite:
            d.start()

    lo[...] = mm(split(t_all[1, :, base].T), (th[1], tl[1]))

    @pl.when(fed)
    def _():
        for a in (3, 4):
            own = own_copies(lambda h: chunk(a, p, c, h), a)
            n = len(own) // pieces(a)
            for h in range(pieces(a)):
                arrived(a, p, c, h)
                start(own[h * n:(h + 1) * n])
        for a in (3, 4):
            forward(a)
            finish(a)
        drain()
        zh[...], zl[...] = split(sbuf[...])
        left = mm(split(mf[:, base].T), (zh[...], zl[...]))
        sc[...] = sc[...] + mm(split(left), (mh[...], ml[...]))
        left = mm(split(wf[1, :, base].T), (zh[...], zl[...]))
        lo[...] = lo[...] + mm(split(left), (wh[1], wl[1]))

        def fold(i, _):
            at = pl.ds(pl.multiple_of(i * LANES, LANES), LANES)
            m = split(mbuf[at, :])
            folded[0, at, :] = mm(m, (mh[...], ml[...]))
            folded[1, at, :] = mm(m, (wh[1], wl[1]))
            return 0

        lax.fori_loop(0, B // LANES, fold, 0)

        def place(i, _):
            at = pl.ds(pl.multiple_of(i * LANES, LANES), LANES)
            mf[at, :] = folded[0, at, :]
            mh[at, :], ml[at, :] = split(folded[0, at, :])
            wf[1, at, :] = folded[1, at, :]
            wh[1, at, :], wl[1, at, :] = split(folded[1, at, :])
            return 0

        lax.fori_loop(0, B // LANES, place, 0)

    @pl.when(jnp.logical_not(top))
    def _():
        own = own_copies(lambda h: chunk(2, p, c, h), 2)
        n = len(own) // pieces(2)
        for h in range(pieces(2)):
            arrived(2, p, c, h)

            @pl.when(feeds)
            def _():
                relay[h][0].start()

            start(own[h * n:(h + 1) * n])

        @pl.when(feeds)
        def _():
            for h in range(pieces(2)):
                for d in relay[h][1:]:
                    d.start()

        forward(2, direct=True)
        finish(2)
        drain()

    zh[...], zl[...] = split(zbuf[...])

    moved = mm(split(mf[:, base].T), (zh[...], zl[...]))
    zes[...] = sc[...] + mm(split(moved), (mh[...], ml[...]))

    @pl.when(sends_z)
    def _():
        for d in down:
            d.start()

    rows = pl.ds(pl.multiple_of(off, 8), R)

    @pl.when(p == 0)
    def _():
        out[0] = zes[rows, :]

    @pl.when(p == 1)
    def _():
        step = mm(split(wf[1, :, base].T), (zh[...], zl[...]))
        lo[...] = lo[...] + mm(split(step), (wh[1], wl[1]))
        out[0] = lo[rows, :]

    for d in outer:
        d.wait_send()

    @pl.when(sends_z)
    def _():
        for d in down:
            d.wait_send()

    @pl.when(feeds)
    def _():
        for d in composite + sum(relay, []):
            d.wait_send()


def solution(mesh):
    rows_n, cols_n = mesh.shape["row"], mesh.shape["col"]

    def on_device(t, s, e):
        R, B = t.shape[1], t.shape[2]
        ny = cols_n // 2
        sends = 12 * (2 * (ny + 1) + (ny - 1) + 2 + 5 * (ny - 1)) + 8 * (ny + 1)
        vmem = pl.BlockSpec(memory_space=pltpu.VMEM)
        V = pltpu.VMEM
        return pl.pallas_call(
            functools.partial(kernel, rows_n, cols_n),
            out_shape=jax.ShapeDtypeStruct(t.shape, F32),
            in_specs=[vmem] * 3,
            out_specs=vmem,
            scratch_shapes=[
                V((2, B, B), F32), V((2, B, B), F32), V((B, B), F32),
                V((2, B, B), BF16), V((2, B, B), BF16),
                V((2, B, B), F32), V((2, B, B), BF16), V((2, B, B), BF16),
                V((B, B), F32), V((B, B), BF16), V((B, B), BF16),
                V((B, B), BF16), V((B, B), BF16),
                V((LANES, B), F32), V((LANES, B), F32), V((LANES, B), F32),
                V((B, B), F32), V((B, B), F32), V((2, B, B), F32),
                pltpu.SemaphoreType.DMA((sends,)),
                pltpu.SemaphoreType.DMA((5, 2, cols_n, 4)),
                pltpu.SemaphoreType.DMA((3,)),
            ],
            compiler_params=pltpu.CompilerParams(collective_id=0, has_side_effects=True,
                                                 vmem_limit_bytes=56 * 2**20),
        )(t, s, e)

    return jax.shard_map(
        on_device, mesh=mesh,
        in_specs=(P("row", "col", None), P("row", "col", None), P("col", None)),
        out_specs=P("row", "col", None), check_vma=False)
```

```python
import functools
import jax
import jax.numpy as jnp
from jax import lax
from jax.experimental import pallas as pl
from jax.experimental.pallas import tpu as pltpu
from jax.sharding import PartitionSpec as P

MESH = pl.DeviceIdType.MESH
F32 = jnp.float32
BF16 = jnp.bfloat16
LANES = 128


def split(x):
    high = x.astype(BF16)
    return high, (x - high.astype(F32)).astype(BF16)


def mm(a, b, transposed=False):
    (ah, al), (bh, bl) = a, b
    dims = (((1,), (1 if transposed else 0,)), ((), ()))
    dot = lambda l, r: lax.dot_general(l, r, dims, preferred_element_type=F32)
    m = ah.shape[0]
    both = dot(jnp.concatenate([ah, al], axis=0), bh)
    return both[:m] + (both[m:] + dot(ah, bl))


def kernel(rows_n, cols_n, t_in, s_in, e_in, out, t_all, s_all, zbuf, th, tl, wf, wh, wl,
           mf, mh, ml, zh, zl, sc, lo, zes, mbuf, sbuf, folded, send, recv, local):
    row, c = lax.axis_index("row"), lax.axis_index("col")
    p, level = lax.rem(row, 2), row // 2
    core, y = lax.rem(c, 2), c // 2
    ny = cols_n // 2
    R, B = t_in.shape[1], t_in.shape[2]
    levels = rows_n // 2
    top = level == levels - 1
    other_y = [lax.rem(y + d, ny) for d in range(1, ny)]
    across = (row + 1 - 2 * p, c)
    partner = (row, c + 1 - 2 * core)
    beside = [(row, v * 2 + core) for v in other_y]

    barrier = pltpu.get_barrier_semaphore()
    greet = [across, partner] + beside
    for d in greet:
        pl.semaphore_signal(barrier, inc=1, device_id=d, device_id_type=MESH)

    side = row + 1 - 2 * p
    for step, near in ((-2, level > 0), (2, jnp.logical_not(top))):
        @pl.when(near)
        def _():
            pl.semaphore_signal(barrier, inc=1, device_id=(row + step, c), device_id_type=MESH)
            for d in beside:
                pl.semaphore_signal(barrier, inc=1, device_id=(side + step, d[1]), device_id_type=MESH)

    above, below = levels - 1 - level, level
    peers = (above + levels - 1) // levels + (below + levels - 1) // levels
    pl.semaphore_wait(barrier, len(greet) + peers * (1 + len(beside)))

    bufs = (t_all, s_all, zbuf, mbuf, sbuf)
    odd_level = lax.rem(level, 2) == 1
    feeds = jnp.logical_and(odd_level, jnp.logical_not(top))
    fed = jnp.logical_and(jnp.logical_not(odd_level), level < levels - 2)
    sends_z = jnp.logical_and(level > 0, jnp.logical_not(feeds))

    def pieces(a):
        return 2 if a < 2 else max(2, min(4, R // 16))

    def chunk(a, pp, cc, h):
        if a < 2:
            return bufs[a].at[pp, pl.ds(pl.multiple_of(cc * R + h * (R // 2), 8), R // 2), :]
        n = R // 2 // pieces(a)
        return bufs[a].at[pl.ds(pl.multiple_of(cc * R + pp * (R // 2) + h * n, 8), n), :]

    started = []
    count = [0]

    def copy(src, a, pp, cc, h, dev):
        d = pltpu.make_async_remote_copy(
            src_ref=src, dst_ref=chunk(a, pp, cc, h), send_sem=send.at[count[0]],
            recv_sem=recv.at[a, pp, cc, h], device_id=dev, device_id_type=MESH)
        count[0] += 1
        return d

    def launch(src, a, pp, cc, h, dev):
        d = copy(src, a, pp, cc, h, dev)
        d.start()
        started.append(d)

    def arrived(a, pp, cc, h):
        ref = chunk(a, pp, cc, h)
        pltpu.make_async_remote_copy(
            src_ref=ref, dst_ref=ref, send_sem=send.at[0], recv_sem=recv.at[a, pp, cc, h],
            device_id=partner, device_id_type=MESH).wait_recv()

    def own_copies(src, a):
        return [copy(src(h), a, p, c, h, d) for h in range(pieces(a))
                for d in [across] + beside + [partner]]

    def forward(a, between=lambda: None, direct=False):
        q = 1 - p
        for h in range(pieces(a)):
            arrived(a, q, c, h)
            if h % 2 == 0 and not direct:
                for d in beside:
                    launch(chunk(a, q, c, h), a, q, c, h, d)
            launch(chunk(a, q, c, h), a, q, c, h, partner)
            for d in beside:
                arrived(a, p, d[1], h)
                if h % 2 == 1 and not direct:
                    launch(chunk(a, p, d[1], h), a, p, d[1], h, across)
                launch(chunk(a, p, d[1], h), a, p, d[1], h, partner)
            if h == 0:
                between()

    def finish(a, use=lambda pp, cc: None):
        q = 1 - p
        use(q, c)
        for d in beside:
            use(p, d[1])
        for h in range(pieces(a)):
            for d in beside:
                arrived(a, q, d[1], h)
                launch(chunk(a, q, d[1], h), a, q, d[1], h, partner)
        for pp in (p, q):
            for v in [y] + other_y:
                for h in range(pieces(a)):
                    arrived(a, pp, v * 2 + 1 - core, h)
                use(pp, v * 2 + 1 - core)
        for d in beside:
            use(q, d[1])

    def start(copies):
        for d in copies:
            d.start()
            started.append(d)

    def drain():
        for d in started:
            d.wait_send()
        started.clear()

    t_own = own_copies(lambda h: t_in.at[0, pl.ds(h * (R // 2), R // 2), :], 0)
    s_own = own_copies(lambda h: s_in.at[0, pl.ds(h * (R // 2), R // 2), :], 1)
    half = len(s_own) // 2
    start(t_own)
    here = pl.ds(pl.multiple_of(c * R, 8), R)
    keep = [pltpu.make_async_copy(t_in.at[0], t_all.at[p, here, :], local.at[0]),
            pltpu.make_async_copy(s_in.at[0], s_all.at[p, here, :], local.at[1])]
    for d in keep:
        d.start()
    forward(0, lambda: start(s_own[:half]))
    start(s_own[half:])
    for d in keep:
        d.wait()
    finish(0)
    for k in range(2):
        th[k], tl[k] = split(t_all[k])

    def weight(pp, cc):
        at = pl.ds(pl.multiple_of(cc * R, 8), R)
        w = mm(split(s_all[pp, at, :]), (th[pp], tl[pp]))
        wf[pp, at, :] = w
        wh[pp, at, :], wl[pp, at, :] = split(w)

    weight(p, c)
    forward(1)
    first_own = own_copies(lambda h: chunk(2, p, c, h), 2)

    @pl.when(top)
    def _():
        mine = pltpu.make_async_copy(
            e_in.at[pl.ds(pl.multiple_of(p * (R // 2), 8), R // 2), :],
            zbuf.at[pl.ds(pl.multiple_of(c * R + p * (R // 2), 8), R // 2), :], local.at[2])
        mine.start()
        mine.wait()
        for d in first_own:
            d.start()

    finish(1, weight)
    outer = list(started)
    started.clear()

    def joined(i, _):
        at = pl.ds(pl.multiple_of(i * LANES, LANES), LANES)
        m = mm((wh[1, at, :], wl[1, at, :]), (wh[0], wl[0]))
        mf[at, :] = m
        mh[at, :], ml[at, :] = split(m)
        return 0

    base = pl.ds(pl.multiple_of((c * R) // LANES * LANES, LANES), LANES)
    off = lax.rem(c * R, LANES)

    def sums():
        turned = mm(split(wf[0, :, base].T), (th[1], tl[1]), transposed=True)
        turned = mm(split(turned), (th[1], tl[1]))
        sc[...] = mm(split(turned), (wh[0], wl[0])) + mm(split(t_all[0, :, base].T), (th[0], tl[0]))

    @pl.when(top)
    def _():
        lax.fori_loop(0, B // LANES, joined, 0)
        forward(2)
        sums()
        finish(2)
        started.extend(first_own)
        drain()

    @pl.when(jnp.logical_not(top))
    def _():
        lax.fori_loop(0, B // LANES, joined, 0)
        sums()

    def piece(a, ref, first, h):
        n = R // 2 // pieces(a)
        return ref.at[pl.ds(pl.multiple_of(first + p * (R // 2) + h * n, 8), n), :]

    below_me = (row - 2, c)
    below_diagonal = [(row - 1 - 2 * p, d[1]) for d in beside]
    composite = [copy(piece(a, ref, first, h), a, p, c, h, below_me)
                 for a, ref, first in ((3, mf, c * R), (4, sc, off)) for h in range(pieces(a))]
    relay = [[copy(chunk(2, p, c, h), 2, p, c, h, d) for d in [below_me] + below_diagonal]
             for h in range(pieces(2))]
    down = [copy(piece(2, zes, off, h), 2, p, c, h, d)
            for d in [below_me] + below_diagonal for h in range(pieces(2))]

    @pl.when(feeds)
    def _():
        for d in composite:
            d.start()

    def odd_sum():
        lo[...] = mm(split(t_all[1, :, base].T), (th[1], tl[1]))

    pl.when(jnp.logical_not(top))(odd_sum)

    @pl.when(fed)
    def _():
        for a in (3, 4):
            own = own_copies(lambda h: chunk(a, p, c, h), a)
            n = len(own) // pieces(a)
            for h in range(pieces(a)):
                arrived(a, p, c, h)
                start(own[h * n:(h + 1) * n])
        for a in (3, 4):
            forward(a)
            finish(a)
        drain()
        zh[...], zl[...] = split(sbuf[...])
        left = mm(split(mf[:, base].T), (zh[...], zl[...]))
        sc[...] = sc[...] + mm(split(left), (mh[...], ml[...]))
        left = mm(split(wf[1, :, base].T), (zh[...], zl[...]))
        lo[...] = lo[...] + mm(split(left), (wh[1], wl[1]))

        def fold(i, _):
            at = pl.ds(pl.multiple_of(i * LANES, LANES), LANES)
            m = split(mbuf[at, :])
            folded[0, at, :] = mm(m, (mh[...], ml[...]))
            folded[1, at, :] = mm(m, (wh[1], wl[1]))
            return 0

        lax.fori_loop(0, B // LANES, fold, 0)

        def place(i, _):
            at = pl.ds(pl.multiple_of(i * LANES, LANES), LANES)
            mf[at, :] = folded[0, at, :]
            mh[at, :], ml[at, :] = split(folded[0, at, :])
            wf[1, at, :] = folded[1, at, :]
            wh[1, at, :], wl[1, at, :] = split(folded[1, at, :])
            return 0

        lax.fori_loop(0, B // LANES, place, 0)

    @pl.when(jnp.logical_not(top))
    def _():
        own = own_copies(lambda h: chunk(2, p, c, h), 2)
        n = len(own) // pieces(2)
        for h in range(pieces(2)):
            arrived(2, p, c, h)

            @pl.when(feeds)
            def _():
                relay[h][0].start()

            start(own[h * n:(h + 1) * n])

        @pl.when(feeds)
        def _():
            for h in range(pieces(2)):
                for d in relay[h][1:]:
                    d.start()

        forward(2, direct=True)
        finish(2)
        drain()

    zh[...], zl[...] = split(zbuf[...])

    moved = mm(split(mf[:, base].T), (zh[...], zl[...]))
    zes[...] = sc[...] + mm(split(moved), (mh[...], ml[...]))

    @pl.when(sends_z)
    def _():
        for d in down:
            d.start()

    pl.when(top)(odd_sum)
    rows = pl.ds(pl.multiple_of(off, 8), R)

    @pl.when(p == 0)
    def _():
        out[0] = zes[rows, :]

    @pl.when(p == 1)
    def _():
        step = mm(split(wf[1, :, base].T), (zh[...], zl[...]))
        lo[...] = lo[...] + mm(split(step), (wh[1], wl[1]))
        out[0] = lo[rows, :]

    for d in outer:
        d.wait_send()

    @pl.when(sends_z)
    def _():
        for d in down:
            d.wait_send()

    @pl.when(feeds)
    def _():
        for d in composite + sum(relay, []):
            d.wait_send()


def solution(mesh):
    rows_n, cols_n = mesh.shape["row"], mesh.shape["col"]

    def on_device(t, s, e):
        R, B = t.shape[1], t.shape[2]
        ny = cols_n // 2
        sends = 12 * (2 * (ny + 1) + (ny - 1) + 2 + 5 * (ny - 1)) + 8 * (ny + 1)
        vmem = pl.BlockSpec(memory_space=pltpu.VMEM)
        V = pltpu.VMEM
        return pl.pallas_call(
            functools.partial(kernel, rows_n, cols_n),
            out_shape=jax.ShapeDtypeStruct(t.shape, F32),
            in_specs=[vmem] * 3,
            out_specs=vmem,
            scratch_shapes=[
                V((2, B, B), F32), V((2, B, B), F32), V((B, B), F32),
                V((2, B, B), BF16), V((2, B, B), BF16),
                V((2, B, B), F32), V((2, B, B), BF16), V((2, B, B), BF16),
                V((B, B), F32), V((B, B), BF16), V((B, B), BF16),
                V((B, B), BF16), V((B, B), BF16),
                V((LANES, B), F32), V((LANES, B), F32), V((LANES, B), F32),
                V((B, B), F32), V((B, B), F32), V((2, B, B), F32),
                pltpu.SemaphoreType.DMA((sends,)),
                pltpu.SemaphoreType.DMA((5, 2, cols_n, 4)),
                pltpu.SemaphoreType.DMA((3,)),
            ],
            compiler_params=pltpu.CompilerParams(collective_id=0, has_side_effects=True,
                                                 vmem_limit_bytes=56 * 2**20),
        )(t, s, e)

    return jax.shard_map(
        on_device, mesh=mesh,
        in_specs=(P("row", "col", None), P("row", "col", None), P("col", None)),
        out_specs=P("row", "col", None), check_vma=False)
```
